128 devices in a mesh: data: 1, fsdp: 2 (over core), ep: 64 (over z, y, x).
Axes of the slice: x: 4, y: 4, z: 4, core: 2. Of those that a mesh axis runs over, the one named last changes fastest.
Arguments:
- x_in: bfloat16 [384, 512, 768], P(('data', 'fsdp', 'ep'))
- expert_idx: int32 [384, 512, 1], P(('data', 'fsdp', 'ep'))
- expert_slot: int32 [384, 512, 1], P(('data', 'fsdp', 'ep'))
- expert_gate: bfloat16 [384, 512, 1], P(('data', 'fsdp', 'ep'))
- attn_gain: bfloat16 [768], replicated
- w_qkv: bfloat16 [768, 3, 12, 64], P('fsdp')
- w_out: bfloat16 [12, 64, 768], P('fsdp')
- moe_gain: bfloat16 [768], replicated
- w_gate: bfloat16 [64, 768, 3072], P('ep', 'fsdp')
- w_up: bfloat16 [64, 768, 3072], P('ep', 'fsdp')
- w_down: bfloat16 [64, 3072, 768], P('ep', None, 'fsdp')
Outputs:
- output: bfloat16 [384, 512, 768], P(('data', 'fsdp', 'ep'))
All inputs are finite; a program needn't handle non-finite values.
Results may differ from the reference program's by a relative error of at most 0.00933228.
Values are sent between devices in bfloat16 or wider.
A program may use at most 1 GiB of HBM per device.

```python
import jax
import jax.numpy as jnp
from jax import lax

D_MODEL = 768
N_HEADS = 12
HEAD_DIM = 64
EXPERTS = 64
TOP_K = 1
FFN_DIM = 3072
BATCH_DEV = 3
SEQ_LEN = 512
FSDP_SIZE = 2
EP_SIZE = 64
CAPACITY = 32

N_DEV = FSDP_SIZE * EP_SIZE
BATCH_ROWS = N_DEV * BATCH_DEV
TOK_DEV = BATCH_DEV * SEQ_LEN
COVER_LEN = (EXPERTS + N_DEV - 1) // N_DEV
NORM_EPS = 1e-6
ROPE_BASE = 10000.0


def draw_routing(rng_key):
    key_base, key_perm, key_hot = jax.random.split(rng_key, 3)
    base_score = jax.random.randint(key_base, (N_DEV, TOK_DEV, EXPERTS), 0, 4096)
    skew_bias = jax.random.permutation(key_perm, EXPERTS) * (4096 // EXPERTS)
    hot_expert = jax.random.randint(key_hot, (), 0, EXPERTS)
    expert_ids = jnp.arange(EXPERTS)
    tok_pos = jnp.arange(TOK_DEV)[None, :]
    dev_pos = jnp.arange(N_DEV)[:, None]
    cover_ids = (dev_pos * COVER_LEN + tok_pos - CAPACITY) % EXPERTS
    in_cover = (tok_pos >= CAPACITY) & (tok_pos < CAPACITY + COVER_LEN)
    forced = jnp.where(tok_pos < CAPACITY, hot_expert, jnp.where(in_cover, cover_ids, -1))
    route_score = base_score + skew_bias + 16384 * (forced[:, :, None] == expert_ids).astype(jnp.int32)
    route_score = route_score * EXPERTS + expert_ids
    chosen = lax.top_k(route_score, TOP_K)[1].astype(jnp.int32)

    def slot_one(dev_ids):
        flat_ids = dev_ids.reshape(TOK_DEV * TOP_K)
        hit_mask = (flat_ids[:, None] == expert_ids[None, :]).astype(jnp.int32)
        prior_count = jnp.sum((jnp.cumsum(hit_mask, axis=0) - hit_mask) * hit_mask, axis=1)
        return jnp.where(prior_count < CAPACITY, prior_count, -1).reshape(TOK_DEV, TOP_K)

    slot_vals = lax.map(slot_one, chosen).astype(jnp.int32)
    out_shape = (BATCH_ROWS, SEQ_LEN, TOP_K)
    return chosen.reshape(out_shape), slot_vals.reshape(out_shape)


def setup_inputs(seed: int = 0, part: int = 0) -> dict:
    part_key = jax.random.fold_in(jax.random.key(seed), part)
    key_tokens, key_route, key_weights = jax.random.split(part_key, 3)
    shared = jax.random.split(jax.random.key(seed + 1), 7)
    expert_idx, expert_slot = draw_routing(key_route)
    x_in = jax.random.normal(key_tokens, (BATCH_ROWS, SEQ_LEN, D_MODEL), jnp.float32)
    expert_gate = jax.random.uniform(key_weights, (BATCH_ROWS, SEQ_LEN, TOP_K), jnp.float32, 0.5, 1.5)
    attn_gain = jax.random.uniform(shared[0], (D_MODEL,), jnp.float32, 0.5, 1.5)
    moe_gain = jax.random.uniform(shared[1], (D_MODEL,), jnp.float32, 0.5, 1.5)
    w_qkv = jax.random.normal(shared[2], (D_MODEL, 3, N_HEADS, HEAD_DIM), jnp.float32) * (1.5 * D_MODEL ** -0.5)
    w_out = jax.random.normal(shared[3], (N_HEADS, HEAD_DIM, D_MODEL), jnp.float32) * (N_HEADS * HEAD_DIM) ** -0.5
    w_gate = jax.random.normal(shared[4], (EXPERTS, D_MODEL, FFN_DIM), jnp.float32) * D_MODEL ** -0.5
    w_up = jax.random.normal(shared[5], (EXPERTS, D_MODEL, FFN_DIM), jnp.float32) * D_MODEL ** -0.5
    w_down = jax.random.normal(shared[6], (EXPERTS, FFN_DIM, D_MODEL), jnp.float32) * FFN_DIM ** -0.5
    return {
        'x_in': x_in.astype(jnp.bfloat16),
        'expert_idx': expert_idx,
        'expert_slot': expert_slot,
        'expert_gate': expert_gate.astype(jnp.bfloat16),
        'attn_gain': attn_gain.astype(jnp.bfloat16),
        'w_qkv': w_qkv.astype(jnp.bfloat16),
        'w_out': w_out.astype(jnp.bfloat16),
        'moe_gain': moe_gain.astype(jnp.bfloat16),
        'w_gate': w_gate.astype(jnp.bfloat16),
        'w_up': w_up.astype(jnp.bfloat16),
        'w_down': w_down.astype(jnp.bfloat16),
    }


def rms_norm(hidden, gain_vec):
    wide = hidden.astype(jnp.float32)
    inv_rms = lax.rsqrt(jnp.mean(wide * wide, axis=-1, keepdims=True) + NORM_EPS)
    return (wide * inv_rms * gain_vec.astype(jnp.float32)).astype(jnp.bfloat16)


def rope_tables():
    half_dim = HEAD_DIM // 2
    inv_freq = ROPE_BASE ** (-jnp.arange(half_dim, dtype=jnp.float32) / half_dim)
    angles = jnp.arange(SEQ_LEN, dtype=jnp.float32)[:, None] * inv_freq[None, :]
    return jnp.cos(angles)[:, None, :], jnp.sin(angles)[:, None, :]


def rotate(heads_in, cos_tab, sin_tab):
    half_dim = HEAD_DIM // 2
    first_half = heads_in[..., :half_dim]
    second_half = heads_in[..., half_dim:]
    return jnp.concatenate([first_half * cos_tab - second_half * sin_tab, second_half * cos_tab + first_half * sin_tab], axis=-1)


def attend_one(seq_in, attn_gain, w_qkv, w_out, cos_tab, sin_tab):
    normed = rms_norm(seq_in, attn_gain)
    qkv_proj = jnp.dot(normed, w_qkv.reshape(D_MODEL, 3 * N_HEADS * HEAD_DIM), preferred_element_type=jnp.float32).reshape(SEQ_LEN, 3, N_HEADS, HEAD_DIM)
    query_rot = rotate(qkv_proj[:, 0], cos_tab, sin_tab).astype(jnp.bfloat16).astype(jnp.float32)
    keys_rot = rotate(qkv_proj[:, 1], cos_tab, sin_tab).astype(jnp.bfloat16).astype(jnp.float32)
    values = qkv_proj[:, 2].astype(jnp.bfloat16).astype(jnp.float32)
    scores = jnp.einsum('qhd,khd->hqk', query_rot, keys_rot) * (HEAD_DIM ** -0.5)
    causal = jnp.arange(SEQ_LEN)[:, None] >= jnp.arange(SEQ_LEN)[None, :]
    attn_probs = jax.nn.softmax(jnp.where(causal[None], scores, -1e30), axis=-1).astype(jnp.bfloat16)
    context = jnp.einsum('hqk,khd->qhd', attn_probs.astype(jnp.float32), values).astype(jnp.bfloat16)
    attn_out = jnp.dot(context.reshape(SEQ_LEN, N_HEADS * HEAD_DIM), w_out.reshape(N_HEADS * HEAD_DIM, D_MODEL), preferred_element_type=jnp.float32)
    return (seq_in.astype(jnp.float32) + attn_out).astype(jnp.bfloat16)


def reference(x_in, expert_idx, expert_slot, expert_gate, attn_gain, w_qkv, w_out, moe_gain, w_gate, w_up, w_down):
    cos_tab, sin_tab = rope_tables()
    hidden = lax.map(lambda seq_in: attend_one(seq_in, attn_gain, w_qkv, w_out, cos_tab, sin_tab), x_in)
    normed = rms_norm(hidden, moe_gain).reshape(N_DEV, TOK_DEV, D_MODEL)
    total_slots = EXPERTS * CAPACITY
    dest_pos = jnp.where(expert_slot >= 0, expert_idx * CAPACITY + expert_slot, total_slots).reshape(N_DEV, TOK_DEV * TOP_K)
    gate_flat = expert_gate.astype(jnp.float32).reshape(N_DEV, TOK_DEV * TOP_K)
    tok_index = jnp.broadcast_to(jnp.arange(TOK_DEV)[:, None], (TOK_DEV, TOP_K)).reshape(TOK_DEV * TOP_K)

    def invert(dest_row, gate_row):
        owner_row = jnp.full((total_slots,), TOK_DEV, jnp.int32).at[dest_row].set(tok_index, mode='drop')
        weight_row = jnp.zeros((total_slots,), jnp.float32).at[dest_row].set(gate_row, mode='drop')
        return owner_row, weight_row

    owner_tok, slot_weight = jax.vmap(invert)(dest_pos, gate_flat)
    owner_tok = owner_tok.reshape(N_DEV, EXPERTS, CAPACITY).transpose(1, 0, 2)
    slot_weight = slot_weight.reshape(N_DEV, EXPERTS, CAPACITY).transpose(1, 0, 2)

    def expert_step(moe_acc, step_in):
        owner_e, weight_e, gate_w, up_w, down_w = step_in
        safe_ids = jnp.minimum(owner_e, TOK_DEV - 1)
        tok_rows = jax.vmap(lambda dev_rows, row_ids: dev_rows[row_ids])(normed, safe_ids).reshape(N_DEV * CAPACITY, D_MODEL)
        gate_act = jnp.dot(tok_rows, gate_w, preferred_element_type=jnp.float32)
        up_act = jnp.dot(tok_rows, up_w, preferred_element_type=jnp.float32)
        inner_act = (jax.nn.silu(gate_act) * up_act).astype(jnp.bfloat16)
        expert_out = jnp.dot(inner_act, down_w, preferred_element_type=jnp.float32).astype(jnp.bfloat16)
        contrib = expert_out.astype(jnp.float32).reshape(N_DEV, CAPACITY, D_MODEL) * weight_e[:, :, None]
        moe_acc = jax.vmap(lambda acc_rows, row_ids, add_rows: acc_rows.at[row_ids].add(add_rows, mode='drop'))(moe_acc, owner_e, contrib)
        return moe_acc, None

    moe_sum = lax.scan(expert_step, jnp.zeros((N_DEV, TOK_DEV, D_MODEL), jnp.float32), (owner_tok, slot_weight, w_gate, w_up, w_down))[0]
    result = hidden.astype(jnp.float32) + moe_sum.reshape(BATCH_ROWS, SEQ_LEN, D_MODEL)
    return result.astype(jnp.bfloat16)
```

```python
import functools

import jax
import jax.numpy as jnp
from jax import lax
from jax.experimental import pallas as pl
from jax.experimental.pallas import tpu as pltpu
from jax.sharding import PartitionSpec as P

MESH = pl.DeviceIdType.MESH
NORM_EPS = 1e-6
ROPE_BASE = 10000.0
N_EP = 64
CAP = 32
GROUP = 8
GROWS = GROUP * CAP
N_GROUPS = N_EP // GROUP
TOK = 1536
TTILE = 512
FFN = 3072
FTILE = 512


def rms_norm(hidden, gain_vec):
    wide = hidden.astype(jnp.float32)
    inv_rms = lax.rsqrt(jnp.mean(wide * wide, axis=-1, keepdims=True) + NORM_EPS)
    return (wide * inv_rms * gain_vec.astype(jnp.float32)).astype(jnp.bfloat16)


def attention_block(x_blk, attn_gain, w_qkv, w_out):
    seq_len = x_blk.shape[1]
    head_dim = w_qkv.shape[3]
    half_dim = head_dim // 2
    normed = rms_norm(x_blk, attn_gain)
    qkv_proj = jnp.einsum('bsd,dthe->bsthe', normed, w_qkv, preferred_element_type=jnp.float32)
    inv_freq = ROPE_BASE ** (-jnp.arange(half_dim, dtype=jnp.float32) / half_dim)
    angles = jnp.arange(seq_len, dtype=jnp.float32)[:, None] * inv_freq[None, :]
    cos_tab = jnp.cos(angles)[None, :, None, :]
    sin_tab = jnp.sin(angles)[None, :, None, :]

    def rotate(heads_in):
        first_half = heads_in[..., :half_dim]
        second_half = heads_in[..., half_dim:]
        return jnp.concatenate([first_half * cos_tab - second_half * sin_tab, second_half * cos_tab + first_half * sin_tab], axis=-1)

    query_rot = rotate(qkv_proj[:, :, 0]).astype(jnp.bfloat16)
    keys_rot = rotate(qkv_proj[:, :, 1]).astype(jnp.bfloat16)
    values = qkv_proj[:, :, 2].astype(jnp.bfloat16)
    scores = jnp.einsum('bqhe,bkhe->bhqk', query_rot, keys_rot, preferred_element_type=jnp.float32) * (head_dim ** -0.5)
    causal = jnp.arange(seq_len)[:, None] >= jnp.arange(seq_len)[None, :]
    attn_probs = jax.nn.softmax(jnp.where(causal, scores, -1e30), axis=-1).astype(jnp.bfloat16)
    context = jnp.einsum('bhqk,bkhe->bqhe', attn_probs, values, preferred_element_type=jnp.float32).astype(jnp.bfloat16)
    attn_out = jnp.einsum('crif,ife->cre', context, w_out, preferred_element_type=jnp.float32)
    return (x_blk.astype(jnp.float32) + attn_out).astype(jnp.bfloat16)


def moe_kernel(u_ref, h_ref, drow_ref, dcol_ref, gcol_ref, wg_hbm, wu_hbm, wd_hbm, out_ref,
               send, recv, ybuf, back, wg, wu, wd, act, acc,
               w_local, w_send, w_recv, out_send, out_recv, ret_send, ret_recv):
    fs = lax.axis_index('fsdp')
    ep = lax.axis_index('ep')
    me = (lax.rem(ep, 4), lax.rem(ep // 4, 4), ep // 16)
    half = wg_hbm.shape[1]

    def peer(k, sign):
        offs = (lax.rem(k, 4), lax.rem(k // 4, 4), k // 16)
        px, py, pz = [lax.rem(m + sign * o + 4, 4) for m, o in zip(me, offs)]
        return pz * 16 + py * 4 + px

    def slot_ids(k_of_row, c_of_row):
        ex = (me[0] + k_of_row) & 3
        ey = (me[1] + (k_of_row >> 2)) & 3
        ez = (me[2] + (k_of_row >> 4)) & 3
        return (ez * 16 + ey * 4 + ex) * CAP + c_of_row

    barrier = pltpu.get_barrier_semaphore()
    pl.semaphore_signal(barrier, inc=1, device_id=(0, 1 - fs, ep), device_id_type=MESH)

    @pl.loop(1, N_EP)
    def _(k):
        pl.semaphore_signal(barrier, inc=1, device_id=(0, fs, peer(k, 1)), device_id_type=MESH)

    lo = pl.multiple_of(fs * half, half)
    weight_views = (
        (wg_hbm.at[0], wg.at[pl.ds(lo, half)]),
        (wu_hbm.at[0], wu.at[pl.ds(lo, half)]),
        (wd_hbm.at[0], wd.at[:, pl.ds(lo, half)]),
    )
    local_copies = [pltpu.make_async_copy(src, dst, w_local.at[i]) for i, (src, dst) in enumerate(weight_views)]
    remote_copies = [
        pltpu.make_async_remote_copy(src_ref=src, dst_ref=dst, send_sem=w_send.at[i], recv_sem=w_recv.at[i], device_id=(0, 1 - fs, ep), device_id_type=MESH)
        for i, (src, dst) in enumerate(weight_views)
    ]
    for copy in local_copies:
        copy.start()
    pl.semaphore_wait(barrier, N_EP)
    for copy in remote_copies:
        copy.start()

    def out_copy(k):
        rows = pl.ds(pl.multiple_of(k * CAP, CAP), CAP)
        return pltpu.make_async_remote_copy(
            src_ref=send.at[rows], dst_ref=recv.at[rows], send_sem=out_send.at[k], recv_sem=out_recv.at[k],
            device_id=(0, fs, peer(k, 1)), device_id_type=MESH)

    def ret_copy(k):
        rows = pl.ds(pl.multiple_of(k * CAP, CAP), CAP)
        return pltpu.make_async_remote_copy(
            src_ref=ybuf.at[rows], dst_ref=back.at[rows], send_sem=ret_send.at[k], recv_sem=ret_recv.at[k],
            device_id=(0, fs, peer(k, -1)), device_id_type=MESH)

    def each(g, act_on):
        for j in range(GROUP):
            k = g * GROUP + j
            if j == 0:
                pl.when(k > 0)(functools.partial(act_on, k))
            else:
                act_on(k)

    @pl.loop(0, N_GROUPS)
    def _(g):
        row = lax.broadcasted_iota(jnp.int32, (GROWS, 1), 0)
        sid = slot_ids(g * GROUP + (row >> 5), row & (CAP - 1))
        pick = jnp.where(sid == drow_ref[...], 1.0, 0.0).astype(jnp.bfloat16)
        rows = jnp.dot(pick, u_ref[...], preferred_element_type=jnp.float32)
        send[pl.ds(pl.multiple_of(g * GROWS, GROWS), GROWS)] = rows.astype(jnp.bfloat16)
        each(g, lambda k: out_copy(k).start())

    recv[pl.ds(0, CAP)] = send[pl.ds(0, CAP)]
    for copy in local_copies:
        copy.wait()
    for copy in remote_copies:
        copy.wait_recv()

    @pl.loop(0, N_GROUPS)
    def _(g):
        each(g, lambda k: out_copy(k).wait_recv())
        here = pl.ds(pl.multiple_of(g * GROWS, GROWS), GROWS)

        @pl.loop(0, FFN // FTILE)
        def _(t):
            cols = pl.ds(pl.multiple_of(t * FTILE, FTILE), FTILE)
            gate_act = jnp.dot(recv[here], wg[:, cols], preferred_element_type=jnp.float32)
            up_act = jnp.dot(recv[here], wu[:, cols], preferred_element_type=jnp.float32)
            act[:, cols] = (jax.nn.silu(gate_act) * up_act).astype(jnp.bfloat16)

        ybuf[here] = jnp.dot(act[...], wd[...], preferred_element_type=jnp.float32).astype(jnp.bfloat16)
        each(g, lambda k: ret_copy(k).start())

    back[pl.ds(0, CAP)] = ybuf[pl.ds(0, CAP)]

    def combine(g, first, last):
        each(g, lambda k: ret_copy(k).wait_recv())
        col = lax.broadcasted_iota(jnp.int32, (1, GROWS), 1)
        sid = slot_ids(g * GROUP + (col >> 5), col & (CAP - 1))

        @pl.loop(0, TOK // TTILE)
        def _(i):
            toks = pl.ds(pl.multiple_of(i * TTILE, TTILE), TTILE)
            pick = jnp.where(sid == dcol_ref[toks], gcol_ref[toks], 0.0).astype(jnp.bfloat16)
            part = jnp.dot(pick, back[pl.ds(pl.multiple_of(g * GROWS, GROWS), GROWS)], preferred_element_type=jnp.float32)
            prev = h_ref[toks].astype(jnp.float32) if first else acc[toks]
            if last:
                out_ref[toks] = (prev + part).astype(jnp.bfloat16)
            else:
                acc[toks] = prev + part

    combine(0, True, False)

    @pl.loop(1, N_GROUPS - 1)
    def _(g):
        combine(g, False, False)

    combine(N_GROUPS - 1, False, True)

    for copy in remote_copies:
        copy.wait_send()

    @pl.loop(1, N_EP)
    def _(k):
        out_copy(k).wait_send()
        ret_copy(k).wait_send()


def moe(u, h, dest, gate, wg, wu, wd):
    vmem = pl.BlockSpec(memory_space=pltpu.VMEM)
    hbm = pl.BlockSpec(memory_space=pl.ANY)
    slots, d = N_EP * CAP, u.shape[1]
    dma = pltpu.SemaphoreType.DMA
    return pl.pallas_call(
        moe_kernel,
        out_shape=jax.ShapeDtypeStruct(u.shape, jnp.bfloat16),
        in_specs=[vmem] * 5 + [hbm] * 3,
        out_specs=vmem,
        scratch_shapes=[pltpu.VMEM((slots, d), jnp.bfloat16)] * 4 + [
            pltpu.VMEM((d, FFN), jnp.bfloat16), pltpu.VMEM((d, FFN), jnp.bfloat16), pltpu.VMEM((FFN, d), jnp.bfloat16),
            pltpu.VMEM((GROWS, FFN), jnp.bfloat16), pltpu.VMEM((TOK, d), jnp.float32),
            dma((3,)), dma((3,)), dma((3,)), dma((N_EP,)), dma((N_EP,)), dma((N_EP,)), dma((N_EP,))],
        compiler_params=pltpu.CompilerParams(collective_id=1, has_side_effects=True, vmem_limit_bytes=60 << 20),
        name='moe',
    )(u, h, dest.reshape(1, TOK), dest.reshape(TOK, 1), gate.reshape(TOK, 1), wg, wu, wd)


def solution(mesh):
    tok_spec = P(('data', 'fsdp', 'ep'), None, None)

    def local_step(x_blk, idx_blk, slot_blk, gate_blk, attn_gain, qkv_shard, out_shard, moe_gain, gate_shard, up_shard, down_shard):
        w_qkv = lax.all_gather(qkv_shard, 'fsdp', axis=0, tiled=True)
        w_out = lax.all_gather(out_shard, 'fsdp', axis=0, tiled=True)
        hidden = attention_block(x_blk, attn_gain, w_qkv, w_out)
        batch_rows, seq_len, d_model = x_blk.shape
        dest = jnp.where(slot_blk >= 0, idx_blk * CAP + slot_blk, -1).reshape(TOK)
        normed = rms_norm(hidden, moe_gain).reshape(TOK, d_model)
        result = moe(normed, hidden.reshape(TOK, d_model), dest, gate_blk.astype(jnp.float32), gate_shard, up_shard, down_shard)
        return result.reshape(batch_rows, seq_len, d_model)

    return jax.shard_map(local_step, mesh=mesh, in_specs=(tok_spec, tok_spec, tok_spec, tok_spec, P(None), P('fsdp', None, None, None), P('fsdp', None, None), P(None), P('ep', 'fsdp', None), P('ep', 'fsdp', None), P('ep', None, 'fsdp')), out_specs=tok_spec, check_vma=False)
```

```python
import functools

import jax
import jax.numpy as jnp
import numpy as np
from jax import lax
from jax.experimental import pallas as pl
from jax.experimental.pallas import tpu as pltpu
from jax.sharding import PartitionSpec as P

MESH = pl.DeviceIdType.MESH
NORM_EPS = 1e-6
ROPE_BASE = 10000.0
N_EP = 64
CAP = 32
GROUP = 8
GROWS = GROUP * CAP
N_GROUPS = N_EP // GROUP
SEQS = 3
SEQ = 512
TOK = SEQS * SEQ
TTILE = 512
D = 768
FFN = 3072
FTILE = 512
HEADS = 12
HEAD = 64
QKV = 3 * HEADS * HEAD
QTILE = 256
LANES = 128
F32, BF16 = jnp.float32, jnp.bfloat16


def rows_at(i, size):
    return pl.ds(pl.multiple_of(i * size, size), size)


def norm(wide, gain):
    inv_rms = lax.rsqrt(jnp.mean(wide * wide, axis=-1, keepdims=True) + NORM_EPS)
    return (wide * inv_rms * gain).astype(BF16)


def dot_nt(a, b):
    return lax.dot_general(a, b, (((1,), (1,)), ((), ())), preferred_element_type=F32)


def layer_kernel(x_hbm, idx_ref, slot_ref, gate_ref, again_ref, mgain_ref, cos_hbm, sin_hbm, wqkv_hbm, wo_hbm, wg_hbm, wu_hbm, wd_hbm, out_ref,
                 x, cos, sin, normed, qkv, ctx, h, u, dest, dcol, gcol,
                 send, recv, ybuf, back, wqkv, wo, wg, wu, wd, act,
                 x_sem, t_sem, w_local, w_send, w_recv, out_send, out_recv, ret_send, ret_recv):
    fs = lax.axis_index('fsdp')
    ep = lax.axis_index('ep')
    me = (lax.rem(ep, 4), lax.rem(ep // 4, 4), ep // 16)
    half = D // 2

    def peer(k, sign):
        offs = (lax.rem(k, 4), lax.rem(k // 4, 4), k // 16)
        px, py, pz = [lax.rem(m + sign * o + 4, 4) for m, o in zip(me, offs)]
        return pz * 16 + py * 4 + px

    def slot_ids(k_of_row, c_of_row):
        ex = (me[0] + k_of_row) & 3
        ey = (me[1] + (k_of_row >> 2)) & 3
        ez = (me[2] + (k_of_row >> 4)) & 3
        return (ez * 16 + ey * 4 + ex) * CAP + c_of_row

    barrier = pltpu.get_barrier_semaphore()
    pl.semaphore_signal(barrier, inc=1, device_id=(0, 1 - fs, ep), device_id_type=MESH)

    @pl.loop(1, N_EP)
    def _(k):
        pl.semaphore_signal(barrier, inc=1, device_id=(0, fs, peer(k, 1)), device_id_type=MESH)

    x_copies = [pltpu.make_async_copy(x_hbm.at[pl.ds(b * SEQ, SEQ)], x.at[pl.ds(b * SEQ, SEQ)], x_sem.at[b]) for b in range(SEQS)]
    table_copies = [pltpu.make_async_copy(src, dst, t_sem.at[i]) for i, (src, dst) in enumerate(((cos_hbm, cos), (sin_hbm, sin)))]
    lo = pl.ds(pl.multiple_of(fs * half, half), half)
    weight_views = (
        (wqkv_hbm, wqkv.at[:, lo]),
        (wo_hbm, wo.at[lo]),
        (wg_hbm.at[0], wg.at[lo]),
        (wu_hbm.at[0], wu.at[lo]),
        (wd_hbm.at[0], wd.at[:, lo]),
    )
    local_copies = [pltpu.make_async_copy(src, dst, w_local.at[i]) for i, (src, dst) in enumerate(weight_views)]
    remote_copies = [
        pltpu.make_async_remote_copy(src_ref=src, dst_ref=dst, send_sem=w_send.at[i], recv_sem=w_recv.at[i], device_id=(0, 1 - fs, ep), device_id_type=MESH)
        for i, (src, dst) in enumerate(weight_views)
    ]
    x_copies[0].start()
    local_copies[0].start()
    for copy in x_copies[1:] + table_copies + local_copies[1:]:
        copy.start()

    def out_copy(k):
        rows = rows_at(k, CAP)
        return pltpu.make_async_remote_copy(
            src_ref=send.at[rows], dst_ref=recv.at[rows], send_sem=out_send.at[k], recv_sem=out_recv.at[k],
            device_id=(0, fs, peer(k, 1)), device_id_type=MESH)

    def ret_copy(k):
        rows = rows_at(k, CAP)
        return pltpu.make_async_remote_copy(
            src_ref=ybuf.at[rows], dst_ref=back.at[rows], send_sem=ret_send.at[k], recv_sem=ret_recv.at[k],
            device_id=(0, fs, peer(k, -1)), device_id_type=MESH)

    def each(g, act_on):
        for j in range(GROUP):
            k = g * GROUP + j
            if j == 0:
                pl.when(k > 0)(functools.partial(act_on, k))
            else:
                act_on(k)

    pl.semaphore_wait(barrier, N_EP)
    for copy in remote_copies:
        copy.start()

    dest[...] = jnp.where(slot_ref[...] >= 0, idx_ref[...] * CAP + slot_ref[...], -1)
    for i in range(TOK // LANES):
        b, c = divmod(i * LANES, SEQ)
        dcol[pl.ds(i * LANES, LANES)] = jnp.broadcast_to(dest[:, i * LANES:(i + 1) * LANES], (LANES, LANES)).T
        gcol[pl.ds(i * LANES, LANES)] = jnp.broadcast_to(gate_ref[b:b + 1, c:c + LANES].astype(F32), (LANES, LANES)).T

    again = again_ref[...].astype(F32)
    mgain = mgain_ref[...].astype(F32)
    for b in range(SEQS):
        x_copies[b].wait()
        normed[pl.ds(b * SEQ, SEQ)] = norm(x[pl.ds(b * SEQ, SEQ)].astype(F32), again)
    for copy in table_copies:
        copy.wait()

    local_copies[0].wait()
    remote_copies[0].wait_recv()

    lane = lax.broadcasted_iota(jnp.int32, (1, LANES), 1)
    low_half = (lane & (HEAD - 1)) < HEAD // 2
    first_head = lane < HEAD
    causal = lax.broadcasted_iota(jnp.int32, (QTILE, QTILE), 0) >= lax.broadcasted_iota(jnp.int32, (QTILE, QTILE), 1)

    @pl.loop(0, SEQS)
    def _(b):
        toks = rows_at(b, SEQ)

        @pl.loop(0, 2 * HEADS * HEAD // 256)
        def _(t):
            part = dot_nt(normed[toks], wqkv[rows_at(t, 256)])
            scale = jnp.where(t < HEADS * HEAD // 256, HEAD ** -0.5, 1.0).astype(F32)
            for j in range(256 // LANES):
                v = part[:, j * LANES:(j + 1) * LANES]
                swapped = jnp.where(low_half, pltpu.roll(v, LANES - HEAD // 2, 1), pltpu.roll(v, HEAD // 2, 1))
                rot = (v * cos[...] + swapped * sin[...]) * scale
                qkv[:, rows_at(t * 2 + j, LANES)] = rot.astype(BF16)

        @pl.loop(2 * HEADS * HEAD // 256, QKV // 256)
        def _(t):
            qkv[:, rows_at(t, 256)] = dot_nt(normed[toks], wqkv[rows_at(t, 256)]).astype(BF16)

        @pl.loop(0, HEADS // 2)
        def _(p):
            q_cols, k_cols, v_cols = [rows_at(p + i * (HEADS // 2), LANES) for i in range(3)]
            for i in range(SEQ // QTILE):
                q_pair = qkv[pl.ds(i * QTILE, QTILE), q_cols]
                outs = []
                for head_lanes in (first_head, jnp.logical_not(first_head)):
                    q = jnp.where(head_lanes, q_pair, jnp.zeros((), BF16))
                    scores = [dot_nt(q, qkv[pl.ds(j * QTILE, QTILE), k_cols]) for j in range(i + 1)]
                    scores[i] = jnp.where(causal, scores[i], -1e30)
                    top = functools.reduce(jnp.maximum, [jnp.max(s, axis=-1, keepdims=True) for s in scores])
                    exps = [jnp.exp(s - top) for s in scores]
                    inv = 1.0 / sum(jnp.sum(e, axis=-1, keepdims=True) for e in exps)
                    outs.append(sum(
                        jnp.dot((e * inv).astype(BF16), qkv[pl.ds(j * QTILE, QTILE), v_cols], preferred_element_type=F32)
                        for j, e in enumerate(exps)))
                ctx[pl.ds(i * QTILE, QTILE), rows_at(p, LANES)] = jnp.where(first_head, outs[0], outs[1]).astype(BF16)

        @pl.when(b == 0)
        def _():
            local_copies[1].wait()
            remote_copies[1].wait_recv()

        attn = jnp.dot(ctx[...], wo[...], preferred_element_type=F32)
        hidden = (x[toks].astype(F32) + attn).astype(BF16)
        h[toks] = hidden
        u[toks] = norm(hidden.astype(F32), mgain)

    @pl.loop(0, N_GROUPS)
    def _(g):
        row = lax.broadcasted_iota(jnp.int32, (GROWS, 1), 0)
        sid = slot_ids(g * GROUP + (row >> 5), row & (CAP - 1))
        pick = jnp.where(sid == dest[...], 1.0, 0.0).astype(BF16)
        send[rows_at(g, GROWS)] = jnp.dot(pick, u[...], preferred_element_type=F32).astype(BF16)
        each(g, lambda k: out_copy(k).start())

    recv[pl.ds(0, CAP)] = send[pl.ds(0, CAP)]
    for copy in local_copies[2:]:
        copy.wait()
    for copy in remote_copies[2:]:
        copy.wait_recv()

    @pl.loop(0, N_GROUPS)
    def _(g):
        each(g, lambda k: out_copy(k).wait_recv())
        here = rows_at(g, GROWS)

        @pl.loop(0, FFN // FTILE)
        def _(t):
            cols = rows_at(t, FTILE)
            gate_act = jnp.dot(recv[here], wg[:, cols], preferred_element_type=F32)
            up_act = jnp.dot(recv[here], wu[:, cols], preferred_element_type=F32)
            act[:, cols] = (jax.nn.silu(gate_act) * up_act).astype(BF16)

        ybuf[here] = jnp.dot(act[...], wd[...], preferred_element_type=F32).astype(BF16)
        each(g, lambda k: ret_copy(k).start())

    back[pl.ds(0, CAP)] = ybuf[pl.ds(0, CAP)]

    def combine(g, so_far):
        each(g, lambda k: ret_copy(k).wait_recv())
        col = lax.broadcasted_iota(jnp.int32, (1, GROWS), 1)
        sid = slot_ids(g * GROUP + (col >> 5), col & (CAP - 1))

        @pl.loop(0, TOK // TTILE)
        def _(i):
            toks = rows_at(i, TTILE)
            pick = jnp.concatenate([
                jnp.where(sid[:, j * LANES:(j + 1) * LANES] == dcol[toks], gcol[toks], 0.0).astype(BF16)
                for j in range(GROWS // LANES)], axis=1)
            part = jnp.dot(pick, back[rows_at(g, GROWS)], preferred_element_type=F32)
            out_ref[toks] = (so_far[toks].astype(F32) + part).astype(BF16)

    combine(0, h)

    @pl.loop(1, N_GROUPS)
    def _(g):
        combine(g, out_ref)

    for copy in remote_copies:
        copy.wait_send()

    @pl.loop(1, N_EP)
    def _(k):
        out_copy(k).wait_send()
        ret_copy(k).wait_send()


def rope_tables():
    half = HEAD // 2
    inv_freq = np.float32(ROPE_BASE) ** (-np.arange(half, dtype=np.float32) / np.float32(half))
    angles = (np.arange(SEQ, dtype=np.float32)[:, None] * inv_freq[None, :]).astype(np.float64)
    cos, sin = np.cos(angles).astype(np.float32), np.sin(angles).astype(np.float32)
    return np.tile(cos, (1, LANES // half)), np.tile(np.concatenate([-sin, sin], axis=1), (1, LANES // HEAD))


def layer(x, idx, slot, gate, again, mgain, wqkv, wo, wg, wu, wd):
    cos, sin = rope_tables()
    vmem = pl.BlockSpec(memory_space=pltpu.VMEM)
    hbm = pl.BlockSpec(memory_space=pl.ANY)
    dma = pltpu.SemaphoreType.DMA
    slots = N_EP * CAP
    scratch = [
        ((TOK, D), BF16), ((SEQ, LANES), F32), ((SEQ, LANES), F32), ((TOK, D), BF16), ((SEQ, QKV), BF16), ((SEQ, D), BF16),
        ((TOK, D), BF16), ((TOK, D), BF16), ((1, TOK), jnp.int32), ((TOK, LANES), jnp.int32), ((TOK, LANES), F32),
        ((slots, D), BF16), ((slots, D), BF16), ((slots, D), BF16), ((slots, D), BF16),
        ((QKV, D), BF16), ((D, D), BF16), ((D, FFN), BF16), ((D, FFN), BF16), ((FFN, D), BF16), ((GROWS, FFN), BF16),
    ]
    return pl.pallas_call(
        layer_kernel,
        out_shape=jax.ShapeDtypeStruct((TOK, D), BF16),
        in_specs=[hbm] + [vmem] * 5 + [hbm] * 7,
        out_specs=vmem,
        scratch_shapes=[pltpu.VMEM(*s) for s in scratch] + [dma((SEQS,)), dma((2,)), dma((5,)), dma((5,)), dma((5,))] + [dma((N_EP,))] * 4,
        compiler_params=pltpu.CompilerParams(collective_id=1, has_side_effects=True, vmem_limit_bytes=63 << 20),
        name='layer',
    )(x, idx, slot, gate, again, mgain, cos, sin, wqkv, wo, wg, wu, wd)


def solution(mesh):
    tok_spec = P(('data', 'fsdp', 'ep'), None, None)

    def local_step(x_blk, idx_blk, slot_blk, gate_blk, attn_gain, qkv_shard, out_shard, moe_gain, gate_shard, up_shard, down_shard):
        result = layer(
            x_blk.reshape(TOK, D), idx_blk.reshape(1, TOK), slot_blk.reshape(1, TOK), gate_blk.reshape(SEQS, SEQ),
            attn_gain.reshape(1, D), moe_gain.reshape(1, D), qkv_shard.transpose(1, 2, 3, 0).reshape(QKV, D // 2), out_shard.reshape(D // 2, D),
            gate_shard, up_shard, down_shard)
        return result.reshape(x_blk.shape)

    return jax.shard_map(local_step, mesh=mesh, in_specs=(tok_spec, tok_spec, tok_spec, tok_spec, P(None), P('fsdp', None, None, None), P('fsdp', None, None), P(None), P('ep', 'fsdp', None), P('ep', 'fsdp', None), P('ep', None, 'fsdp')), out_specs=tok_spec, check_vma=False)
```

```python
import functools

import jax
import jax.numpy as jnp
import numpy as np
from jax import lax
from jax.experimental import pallas as pl
from jax.experimental.pallas import tpu as pltpu
from jax.sharding import PartitionSpec as P

MESH = pl.DeviceIdType.MESH
NORM_EPS = 1e-6
ROPE_BASE = 10000.0
N_EP = 64
CAP = 32
GROUP = 8
GROWS = GROUP * CAP
N_GROUPS = N_EP // GROUP
SEQS = 3
SEQ = 512
TOK = SEQS * SEQ
TTILE = 512
D = 768
FFN = 3072
FTILE = 512
STRIDE = 27
ETILE = 512
HEADS = 12
HEAD = 64
QKV = 3 * HEADS * HEAD
QTILE = 256
WTILE = 384
LANES = 128
F32, BF16 = jnp.float32, jnp.bfloat16


def rows_at(i, size):
    return pl.ds(pl.multiple_of(i * size, size), size)


def norm(wide, gain):
    inv_rms = lax.rsqrt(jnp.mean(wide * wide, axis=-1, keepdims=True) + NORM_EPS)
    return (wide * inv_rms * gain).astype(BF16)


def dot_nt(a, b):
    return lax.dot_general(a, b, (((1,), (1,)), ((), ())), preferred_element_type=F32)


def layer_kernel(x_hbm, idx_ref, slot_ref, gate_ref, again_ref, mgain_ref, cos_hbm, sin_hbm, wqkv_hbm, wo_hbm, wg_hbm, wu_hbm, wd_hbm,
                 sum_hbm, pick_hbm, last_hbm,
                 x, cos, sin, normed, qkv, ctx, h, u, dest, dcol, gcol,
                 send, recv, ybuf, back, wqkv, wo, wg, wu, wd, act, pick_last,
                 x_sem, t_sem, o_sem, w_local, w_send, w_recv, out_send, out_recv, ret_send, ret_recv):
    fs = lax.axis_index('fsdp')
    ep = lax.axis_index('ep')
    me = (lax.rem(ep, 4), lax.rem(ep // 4, 4), ep // 16)
    half = D // 2

    def peer(i, sign):
        k = lax.rem(i * STRIDE, N_EP)
        offs = (lax.rem(k, 4), lax.rem(k // 4, 4), k // 16)
        px, py, pz = [lax.rem(m + sign * o + 4, 4) for m, o in zip(me, offs)]
        return pz * 16 + py * 4 + px

    def slot_ids(i_of_row, c_of_row):
        k_of_row = (i_of_row * STRIDE) & (N_EP - 1)
        ex = (me[0] + k_of_row) & 3
        ey = (me[1] + (k_of_row >> 2)) & 3
        ez = (me[2] + (k_of_row >> 4)) & 3
        return (ez * 16 + ey * 4 + ex) * CAP + c_of_row

    barrier = pltpu.get_barrier_semaphore()
    pl.semaphore_signal(barrier, inc=1, device_id=(0, 1 - fs, ep), device_id_type=MESH)

    @pl.loop(1, N_EP)
    def _(k):
        pl.semaphore_signal(barrier, inc=1, device_id=(0, fs, peer(k, 1)), device_id_type=MESH)

    x_copies = [pltpu.make_async_copy(x_hbm.at[pl.ds(b * SEQ, SEQ)], x.at[pl.ds(b * SEQ, SEQ)], x_sem.at[b]) for b in range(SEQS)]
    table_copies = [pltpu.make_async_copy(src, dst, t_sem.at[i]) for i, (src, dst) in enumerate(((cos_hbm, cos), (sin_hbm, sin)))]
    lo = pl.ds(pl.multiple_of(fs * half, half), half)
    weight_views = (
        (wqkv_hbm, wqkv.at[:, lo]),
        (wo_hbm, wo.at[lo]),
        (wg_hbm.at[0], wg.at[lo]),
        (wu_hbm.at[0], wu.at[lo]),
        (wd_hbm.at[0], wd.at[:, lo]),
    )
    local_copies = [pltpu.make_async_copy(src, dst, w_local.at[i]) for i, (src, dst) in enumerate(weight_views)]
    remote_copies = [
        pltpu.make_async_remote_copy(src_ref=src, dst_ref=dst, send_sem=w_send.at[i], recv_sem=w_recv.at[i], device_id=(0, 1 - fs, ep), device_id_type=MESH)
        for i, (src, dst) in enumerate(weight_views)
    ]
    x_copies[0].start()
    local_copies[0].start()
    for copy in x_copies[1:] + table_copies + local_copies[1:]:
        copy.start()

    def out_copy(k):
        rows = rows_at(k, CAP)
        return pltpu.make_async_remote_copy(
            src_ref=send.at[rows], dst_ref=recv.at[rows], send_sem=out_send.at[k], recv_sem=out_recv.at[k],
            device_id=(0, fs, peer(k, 1)), device_id_type=MESH)

    def ret_copy(k, last=False):
        rows = rows_at(k, CAP)
        landing = last_hbm.at[rows_at(k - (N_EP - GROUP), CAP)] if last else back.at[rows]
        return pltpu.make_async_remote_copy(
            src_ref=ybuf.at[rows], dst_ref=landing, send_sem=ret_send.at[k], recv_sem=ret_recv.at[k],
            device_id=(0, fs, peer(k, -1)), device_id_type=MESH)

    def each(g, act_on):
        for j in range(GROUP):
            k = g * GROUP + j
            if j == 0:
                pl.when(k > 0)(functools.partial(act_on, k))
            else:
                act_on(k)

    with jax.named_scope('tables'):
        dest[...] = jnp.where(slot_ref[...] >= 0, idx_ref[...] * CAP + slot_ref[...], -1)
        for i in range(TOK // LANES):
            b, c = divmod(i * LANES, SEQ)
            dcol[pl.ds(i * LANES, LANES)] = jnp.broadcast_to(dest[:, i * LANES:(i + 1) * LANES], (LANES, LANES)).T
            gcol[pl.ds(i * LANES, LANES)] = jnp.broadcast_to(gate_ref[b:b + 1, c:c + LANES].astype(F32), (LANES, LANES)).T
    again = again_ref[...].astype(F32).reshape(1, D)
    mgain = mgain_ref[...].astype(F32).reshape(1, D)
    with jax.named_scope('norm_in'):
        for b in range(SEQS):
            x_copies[b].wait()
            normed[pl.ds(b * SEQ, SEQ)] = norm(x[pl.ds(b * SEQ, SEQ)].astype(F32), again)
    with jax.named_scope('barrier'):
        pl.semaphore_wait(barrier, N_EP)
    for copy in remote_copies:
        copy.start()

    for copy in table_copies:
        copy.wait()

    with jax.named_scope('wqkv_wait'):
        local_copies[0].wait()
        remote_copies[0].wait_recv()

    first_head = lax.broadcasted_iota(jnp.int32, (1, LANES), 1) < HEAD
    causal = lax.broadcasted_iota(jnp.int32, (QTILE, QTILE), 0) <= lax.broadcasted_iota(jnp.int32, (QTILE, QTILE), 1)

    @pl.loop(0, SEQS)
    def _(b):
        toks = rows_at(b, SEQ)

        with jax.named_scope('qk'):
            @pl.loop(0, 2 * HEADS * HEAD // WTILE)
            def _(t):
                part = dot_nt(wqkv[rows_at(t, WTILE)], normed[toks])
                which = t // (HEADS * HEAD // WTILE)
                c, s = cos[which], sin[which]
                for j in range(WTILE // HEAD):
                    first, second = part[j * HEAD:j * HEAD + HEAD // 2], part[j * HEAD + HEAD // 2:(j + 1) * HEAD]
                    qkv[pl.ds(pl.multiple_of(t * WTILE + j * HEAD, HEAD), HEAD // 2)] = (first * c - second * s).astype(BF16)
                    qkv[pl.ds(pl.multiple_of(t * WTILE + j * HEAD + HEAD // 2, HEAD // 2), HEAD // 2)] = (second * c + first * s).astype(BF16)

        with jax.named_scope('v'):
            @pl.loop(2 * HEADS * HEAD // WTILE, QKV // WTILE)
            def _(t):
                qkv[rows_at(t, WTILE)] = dot_nt(wqkv[rows_at(t, WTILE)], normed[toks]).astype(BF16)

        with jax.named_scope('attn'):
            @pl.loop(0, HEADS // 2)
            def _(p):
                q_rows, k_rows = rows_at(p, LANES), rows_at(p + HEADS // 2, LANES)
                k_pair = qkv[k_rows].T
                for hh in range(2):
                    k = jnp.where(first_head if hh == 0 else jnp.logical_not(first_head), k_pair, jnp.zeros((), BF16))
                    v = qkv[pl.ds(pl.multiple_of(2 * HEADS * HEAD + p * LANES + hh * HEAD, HEAD), HEAD)]
                    for i in range(SEQ // QTILE):
                        scores = [jnp.dot(k[j * QTILE:(j + 1) * QTILE], qkv[q_rows, pl.ds(i * QTILE, QTILE)], preferred_element_type=F32) for j in range(i + 1)]
                        scores[i] = jnp.where(causal, scores[i], -1e30)
                        top = functools.reduce(jnp.maximum, [jnp.max(s, axis=0, keepdims=True) for s in scores])
                        exps = [jnp.exp(s - top) for s in scores]
                        inv = 1.0 / sum(jnp.sum(e, axis=0, keepdims=True) for e in exps)
                        out = sum(
                            jnp.dot(v[:, j * QTILE:(j + 1) * QTILE], (e * inv).astype(BF16), preferred_element_type=F32)
                            for j, e in enumerate(exps))
                        ctx[pl.ds(pl.multiple_of(p * LANES + hh * HEAD, HEAD), HEAD), pl.ds(i * QTILE, QTILE)] = out.astype(BF16)

        @pl.when(b == 0)
        def _():
            local_copies[1].wait()
            remote_copies[1].wait_recv()

        with jax.named_scope('proj'):
            attn = lax.dot_general(ctx[...], wo[...], (((0,), (0,)), ((), ())), preferred_element_type=F32)
            hidden = (x[toks].astype(F32) + attn).astype(BF16)
            h[toks] = hidden
            u[toks] = norm(hidden.astype(F32), mgain)
    @pl.loop(0, N_GROUPS)
    def _(g):
        with jax.named_scope('dispatch'):
            row = lax.broadcasted_iota(jnp.int32, (GROWS, 1), 0)
            sid = slot_ids(g * GROUP + (row >> 5), row & (CAP - 1))
            pick = jnp.where(sid == dest[...], 1.0, 0.0).astype(BF16)
            send[rows_at(g, GROWS)] = jnp.dot(pick, u[...], preferred_element_type=F32).astype(BF16)
            each(g, lambda k: out_copy(k).start())
    recv[pl.ds(0, CAP)] = send[pl.ds(0, CAP)]
    with jax.named_scope('w_wait'):
        for copy in local_copies[2:]:
            copy.wait()
        for copy in remote_copies[2:]:
            copy.wait_recv()
    def experts(g, last=False):
        with jax.named_scope('ffn_wait'):
            each(g, lambda k: out_copy(k).wait_recv())
        here = rows_at(g, GROWS)

        with jax.named_scope('ffn_up'):
            @pl.loop(0, FFN // FTILE)
            def _(t):
                cols = rows_at(t, FTILE)
                gate_act = jnp.dot(recv[here], wg[:, cols], preferred_element_type=F32)
                up_act = jnp.dot(recv[here], wu[:, cols], preferred_element_type=F32)
                act[:, cols] = (jax.nn.silu(gate_act) * up_act).astype(BF16)

        with jax.named_scope('ffn_down'):
            ybuf[here] = jnp.dot(act[...], wd[...], preferred_element_type=F32).astype(BF16)
            each(g, lambda k: ret_copy(k, last).start())

    @pl.loop(0, N_GROUPS - 1)
    def _(g):
        experts(g)

    experts(jnp.int32(N_GROUPS - 1), True)
    back[pl.ds(0, CAP)] = ybuf[pl.ds(0, CAP)]

    def pick_of(g, toks):
        col = lax.broadcasted_iota(jnp.int32, (1, GROWS), 1)
        sid = slot_ids(g * GROUP + (col >> 5), col & (CAP - 1))
        return jnp.concatenate([
            jnp.where(sid[:, j * LANES:(j + 1) * LANES] == dcol[toks], gcol[toks], 0.0).astype(BF16)
            for j in range(GROWS // LANES)], axis=1)

    pick_last[...] = pick_of(N_GROUPS - 1, pl.ds(0, TOK))
    pick_out = pltpu.make_async_copy(pick_last, pick_hbm, o_sem.at[0])
    pick_out.start()

    @pl.loop(0, N_GROUPS - 1)
    def _(g):
        with jax.named_scope('comb_wait'):
            each(g, lambda k: ret_copy(k).wait_recv())
        with jax.named_scope('comb'):
            @pl.loop(0, TOK // TTILE)
            def _(i):
                toks = rows_at(i, TTILE)
                part = jnp.dot(pick_of(g, toks), back[rows_at(g, GROWS)], preferred_element_type=F32)
                h[toks] = (h[toks].astype(F32) + part).astype(BF16)

    sum_out = pltpu.make_async_copy(h, sum_hbm, o_sem.at[1])
    sum_out.start()

    for copy in remote_copies:
        copy.wait_send()

    @pl.loop(1, N_EP)
    def _(k):
        out_copy(k).wait_send()

    @pl.loop(1, N_EP - GROUP)
    def _(k):
        ret_copy(k).wait_send()

    pick_out.wait()
    sum_out.wait()
    with jax.named_scope('last_wait'):
        @pl.loop(N_EP - GROUP, N_EP)
        def _(k):
            ret_copy(k, True).wait_recv()
            ret_copy(k, True).wait_send()


def finish_kernel(sum_ref, pick_ref, last_ref, out_ref):
    part = jnp.dot(pick_ref[...], last_ref[...], preferred_element_type=F32)
    out_ref[...] = (sum_ref[...].astype(F32) + part).astype(BF16)


def rope_tables():
    half = HEAD // 2
    inv_freq = np.float32(ROPE_BASE) ** (-np.arange(half, dtype=np.float32) / np.float32(half))
    angles = (inv_freq[:, None] * np.arange(SEQ, dtype=np.float32)[None, :]).astype(np.float64)
    scale = np.float32(HEAD ** -0.5)
    return [np.stack([table * scale, table]) for table in (np.cos(angles).astype(np.float32), np.sin(angles).astype(np.float32))]


def layer(x, idx, slot, gate, again, mgain, wqkv, wo, wg, wu, wd):
    cos, sin = rope_tables()
    vmem = pl.BlockSpec(memory_space=pltpu.VMEM)
    hbm = pl.BlockSpec(memory_space=pl.ANY)
    dma = pltpu.SemaphoreType.DMA
    slots = N_EP * CAP
    scratch = [
        ((TOK, D), BF16), ((2, HEAD // 2, SEQ), F32), ((2, HEAD // 2, SEQ), F32), ((TOK, D), BF16), ((QKV, SEQ), BF16), ((D, SEQ), BF16),
        ((TOK, D), BF16), ((TOK, D), BF16), ((1, TOK), jnp.int32), ((TOK, LANES), jnp.int32), ((TOK, LANES), F32),
        ((slots, D), BF16), ((slots, D), BF16), ((slots, D), BF16), ((slots, D), BF16),
        ((QKV, D), BF16), ((D, D), BF16), ((D, FFN), BF16), ((D, FFN), BF16), ((FFN, D), BF16), ((GROWS, FFN), BF16), ((TOK, GROWS), BF16),
    ]
    total, pick, last = pl.pallas_call(
        layer_kernel,
        out_shape=[jax.ShapeDtypeStruct((TOK, D), BF16), jax.ShapeDtypeStruct((TOK, GROWS), BF16), jax.ShapeDtypeStruct((GROWS, D), BF16)],
        in_specs=[hbm] + [vmem] * 5 + [hbm] * 7,
        out_specs=[hbm] * 3,
        scratch_shapes=[pltpu.VMEM(*s) for s in scratch] + [dma((SEQS,)), dma((2,)), dma((2,)), dma((5,)), dma((5,)), dma((5,))] + [dma((N_EP,))] * 4,
        compiler_params=pltpu.CompilerParams(collective_id=1, has_side_effects=True, vmem_limit_bytes=63 << 20),
        name='layer',
    )(x, idx, slot, gate, again, mgain, cos, sin, wqkv, wo, wg, wu, wd)
    return pl.pallas_call(
        finish_kernel,
        grid=(TOK // ETILE,),
        out_shape=jax.ShapeDtypeStruct((TOK, D), BF16),
        in_specs=[pl.BlockSpec((ETILE, D), lambda i: (i, 0)), pl.BlockSpec((ETILE, GROWS), lambda i: (i, 0)), pl.BlockSpec((GROWS, D), lambda i: (0, 0))],
        out_specs=pl.BlockSpec((ETILE, D), lambda i: (i, 0)),
        name='finish',
    )(total, pick, last)


def solution(mesh):
    tok_spec = P(('data', 'fsdp', 'ep'), None, None)

    def local_step(x_blk, idx_blk, slot_blk, gate_blk, attn_gain, qkv_shard, out_shard, moe_gain, gate_shard, up_shard, down_shard):
        result = layer(
            x_blk.reshape(TOK, D), idx_blk.reshape(1, TOK), slot_blk.reshape(1, TOK), gate_blk.reshape(SEQS, SEQ),
            attn_gain, moe_gain, qkv_shard.transpose(1, 2, 3, 0).reshape(QKV, D // 2), out_shard.reshape(D // 2, D),
            gate_shard, up_shard, down_shard)
        return result.reshape(x_blk.shape)

    return jax.shard_map(local_step, mesh=mesh, in_specs=(tok_spec, tok_spec, tok_spec, tok_spec, P(None), P('fsdp', None, None, None), P('fsdp', None, None), P(None), P('ep', 'fsdp', None), P('ep', 'fsdp', None), P('ep', None, 'fsdp')), out_specs=tok_spec, check_vma=False)
```
